128 devices in a mesh: fsdp: 16 (over z, y_hi, core), tp: 8 (over x, y_lo).
Axes of the slice: x: 4, y: 4 (y_hi: 2, y_lo: 2; y = y_hi * 2 + y_lo), z: 4, core: 2. Of those that a mesh axis runs over, the one named last changes fastest.
Arguments:
- param: bfloat16 [1, 8192, 8192], P(None, 'fsdp', 'tp'), may hold values from -0.0625 to 0.0625
- grad: bfloat16 [1, 8192, 8192], P(None, 'fsdp', 'tp'), may hold values from -1500 to 1500
- m_codes: bfloat16 [262144, 256], P(('fsdp', 'tp')), may hold values from -1 to 1
- v_codes: bfloat16 [262144, 256], P(('fsdp', 'tp')), may hold values from 0.049804688 to 1
- m_scales: bfloat16 [262144], P(('fsdp', 'tp')), may hold values from 0.0099487305 to 0.099609375
- v_scales: bfloat16 [262144], P(('fsdp', 'tp')), may hold values from 0.0009994507 to 0.099609375
- block_target: int32 [262144], P(('fsdp', 'tp')), may hold values from 0 to 262143, as said below
Outputs:
- new_param: bfloat16 [1, 8192, 8192], P(None, 'fsdp', 'tp')
- new_m_codes: bfloat16 [1, 8192, 8192], P(None, 'fsdp', 'tp')
- new_m_scales: float32 [1, 8192, 32], P(None, 'fsdp', 'tp')
- new_v_codes: bfloat16 [1, 8192, 8192], P(None, 'fsdp', 'tp')
- new_v_scales: float32 [1, 8192, 32], P(None, 'fsdp', 'tp')
The draws below stay inside these ranges and needn't reach their ends.
Inputs may be any that keep to these rules, and one draw needn't show every extreme that they name: block_target is a permutation of 0 to 262143. Of the 2048 saved blocks of one device, exactly 16 have their target on each device of the weights' layout.
All inputs are finite; a program needn't handle non-finite values. Where the reference program divides by a largest or mean magnitude, that divisor is 1e-20 or more.
Results may differ from the reference program's by a relative error of at most 0.001.
Values may be sent and summed in bfloat16 or wider, within the bound.
No kernel may reach another device: no remote copies, remote signals or barrier semaphores. Data moves between devices by JAX's collectives and lax.ppermute only.
A program may use at most 64 MiB of HBM per device.

```python
import math
import jax
import jax.numpy as jnp
from jax import lax

D = 8192
LAYERS = 1
BLOCK = 256
PEERS = 128
NBLK = 262144
BLK_DEV = 2048
PAIR = 16
ROWS_DEV = 512
COLB_DEV = 4
N_TP = 8


def draw_grad(key, part):
    first, second, third = jax.random.split(jax.random.fold_in(key, 11), 3)
    rows = jnp.arange(D, dtype=jnp.float32) / D
    row_spread = jnp.exp(jax.random.uniform(second, (LAYERS, D, 1), jnp.float32, 0.0, jnp.log(10.0)))
    col_spread = jnp.exp(jax.random.uniform(third, (LAYERS, 1, D), jnp.float32, 0.0, jnp.log(10.0)))
    noise = jax.random.truncated_normal(first, -4.0, 4.0, (LAYERS, D, D), jnp.float32)
    rising = jnp.power(3.0, rows)[None, :, None]
    return (noise * rising * row_spread * col_spread).astype(jnp.bfloat16)


def draw_block_target(key, part):
    devices = jnp.arange(PEERS, dtype=jnp.int32)
    row_shard = devices // N_TP
    col_shard = devices % N_TP
    counter = jnp.arange(BLK_DEV, dtype=jnp.int32)
    layer_size = ROWS_DEV * COLB_DEV
    layer_of = counter // layer_size
    within = counter % layer_size
    row_of = within // COLB_DEV
    column_block = within % COLB_DEV
    global_row = row_shard[:, None] * ROWS_DEV + row_of[None, :]
    global_block = col_shard[:, None] * COLB_DEV + column_block[None, :]
    target = (layer_of[None, :] * D + global_row) * (D // BLOCK) + global_block
    first, second = jax.random.split(jax.random.fold_in(key, 23))
    target = jax.random.permutation(first, target, axis=1, independent=True)
    target = target.reshape(PEERS, PEERS, PAIR).transpose(1, 0, 2).reshape(PEERS, BLK_DEV)
    target = jax.random.permutation(second, target, axis=1, independent=True)
    return target.reshape(NBLK).astype(jnp.int32)


def steps_of(key, extent, shards, least, high):
    def one(axis_at, parts):
        heights = jax.random.uniform(jax.random.fold_in(jax.random.fold_in(key, 6), axis_at), (parts,), jnp.float32, least / len(shards), high / len(shards))
        return jnp.repeat(jnp.exp(heights), extent[axis_at] // parts).reshape((-1,) + (1,) * (len(extent) - axis_at - 1))

    gain = one(*shards[0])
    for cut in shards[1:]:
        gain = gain * one(*cut)
    return gain


def centred(rng, shape, deviation, bound, cuts=(), kind=jnp.bfloat16):
    loudness = steps_of(rng, shape, cuts, -0.22, 0.18) if cuts else 1.0
    array = jax.random.normal(rng, shape, jnp.float32) * deviation * loudness
    return jnp.minimum(jnp.maximum(array, -bound), bound).astype(kind)


def setup_inputs(seed: int = 0) -> dict:
    keys = jax.random.split(jax.random.key(seed), 8)
    param = centred(keys[0], (LAYERS, D, D), D ** -0.5, 0.0625, ((1, 16), (2, 8)))
    grad = draw_grad(jax.random.fold_in(keys[7], 71), 0)
    m_codes = jnp.clip(jax.random.uniform(keys[2], (NBLK, BLOCK), jnp.float32, -1.0, 1.0) * steps_of(keys[2], (NBLK, BLOCK), ((0, 128),), -0.4, 0.0), -1.0, 1.0).astype(jnp.bfloat16)
    v_codes = jnp.clip(0.049804688 + 0.9501953 * jax.random.uniform(keys[3], (NBLK, BLOCK), jnp.float32) ** steps_of(keys[3], (NBLK, BLOCK), ((0, 128),), -0.2, 0.2), 0.049804688, 1.0).astype(jnp.bfloat16)
    m_scales = jnp.clip(jnp.exp(math.log(0.099609375) - 2.3038113 * jax.random.uniform(keys[4], (NBLK,), jnp.float32) ** steps_of(keys[4], (NBLK,), ((0, 128),), -0.2, 0.2)), 0.0099487305, 0.099609375).astype(jnp.bfloat16)
    v_scales = jnp.clip(jnp.exp(math.log(0.099609375) - 4.6018058 * jax.random.uniform(keys[5], (NBLK,), jnp.float32) ** steps_of(keys[5], (NBLK,), ((0, 128),), -0.2, 0.2)), 0.0009994507, 0.099609375).astype(jnp.bfloat16)
    block_target = draw_block_target(jax.random.fold_in(keys[7], 71), 0)
    return dict(param=param, grad=grad, m_codes=m_codes, v_codes=v_codes, m_scales=m_scales, v_scales=v_scales, block_target=block_target)


beta_one = 0.9
beta_two = 0.999
step_count = 1000.0
learn_rate = 0.002
clip_level = 0.5
guard = 1e-06
adam_eps = 1e-08

def requantize(values):
    blocks = values.reshape(D, D // BLOCK, BLOCK)
    largest = lax.optimization_barrier(jnp.max(jnp.abs(blocks), axis=-1))
    quantized = (blocks / (largest[..., None] + guard)).astype(jnp.bfloat16)
    return (quantized.reshape(D, D), largest)

def reference(param, grad, m_codes, v_codes, m_scales, v_scales, block_target):
    layer_blocks = D * D // BLOCK
    source = jnp.zeros((NBLK,), jnp.int32).at[block_target.astype(jnp.int32)].set(jnp.arange(NBLK, dtype=jnp.int32))
    square_sum = jnp.zeros((), jnp.float32)
    for layer_index in range(LAYERS):
        values = grad[layer_index].astype(jnp.float32)
        square_sum = square_sum + jnp.sum(values * values)
    root_mean = jnp.sqrt(square_sum / (LAYERS * D * D) + guard)
    factor = jnp.minimum(1.0, clip_level / root_mean)
    params_out, m_out, ms_out, v_out, vs_out = ([], [], [], [], [])
    for layer_index in range(LAYERS):
        picked = source[layer_index * layer_blocks:(layer_index + 1) * layer_blocks]
        m_prev = (m_codes[picked].astype(jnp.float32) * m_scales[picked].astype(jnp.float32)[:, None]).reshape(D, D)
        v_prev = (v_codes[picked].astype(jnp.float32) * v_scales[picked].astype(jnp.float32)[:, None]).reshape(D, D)
        clipped = grad[layer_index].astype(jnp.float32) * factor
        m_next = beta_one * m_prev + (1.0 - beta_one) * clipped
        v_next = beta_two * v_prev + (1.0 - beta_two) * clipped * clipped
        update = m_next / (1.0 - beta_one ** step_count) / (jnp.sqrt(v_next / (1.0 - beta_two ** step_count)) + adam_eps)
        params_out.append((param[layer_index].astype(jnp.float32) - learn_rate * update).astype(jnp.bfloat16))
        m_quant, m_large = requantize(m_next)
        v_quant, v_large = requantize(v_next)
        m_out.append(m_quant)
        ms_out.append(m_large)
        v_out.append(v_quant)
        vs_out.append(v_large)
    return (jnp.stack(params_out), jnp.stack(m_out), jnp.stack(ms_out), jnp.stack(v_out), jnp.stack(vs_out))
```

```python
import functools

import jax
import jax.numpy as jnp
from jax import lax
from jax.experimental import pallas as pl
from jax.experimental.pallas import tpu as pltpu
from jax.sharding import Mesh
from jax.sharding import PartitionSpec as P

D = 8192
LAYERS = 1
BLOCK = 256
FSDP = ("fsdp_0", "fsdp_1", "fsdp_2")
TP = ("tp_0", "tp_1")
FSDP_TP = ("fsdp_0", "fsdp_1", "fsdp_2", "tp_0", "tp_1")

PEERS = 128
PAIR = 16
SAVED = 2048
ROWS = 512
COLB = 4
N_TP = 8
LANES = 128
CHUNKS = SAVED // LANES
HALVES = BLOCK // LANES
MSG_ROWS = PAIR * HALVES
SIDE = 8

beta_one = 0.9
beta_two = 0.999
step_count = 1000.0
learn_rate = 0.002
clip_level = 0.5
guard = 1e-06
adam_eps = 1e-08

F32 = jnp.float32
BF16 = jnp.bfloat16
INTERPRET = False


def iota(shape, dim):
    return lax.broadcasted_iota(jnp.int32, shape, dim)


def one_hot(condition):
    return jnp.where(condition, 1.0, 0.0).astype(BF16)


def times(a, b):
    return jnp.dot(a, b, preferred_element_type=F32)


def picked_rows(slot_rows, base, count, weights=None):
    wanted = iota((count, LANES), 0) + base
    parts = []
    for k in range(CHUNKS):
        hit = wanted == slot_rows[k]
        weight = 1.0 if weights is None else weights[k]
        parts.append(jnp.where(hit, weight, 0.0).astype(BF16))
    return jnp.concatenate(parts, axis=1)


def fill_message(msg_ref, slot_rows, codes_ref, tile=512):
    codes = codes_ref[...]
    for t in range(SAVED // tile):
        rows = times(picked_rows(slot_rows, t * tile, tile), codes).astype(BF16)
        first = t * tile // PAIR
        for j in range(HALVES):
            msg_ref[pl.ds(first, tile // PAIR), pl.ds(j * PAIR, PAIR), :] = rows[
                :, j * LANES : (j + 1) * LANES
            ].reshape(tile // PAIR, PAIR, LANES)


def prepare_m(target_ref, ms_ref, vs_ref, grad_ref, codes_ref, msg_ref, slot_ref):
    target = target_ref[...]
    row = lax.shift_right_logical(target, 5)
    column = target & (D // BLOCK - 1)
    dest = lax.shift_right_logical(row, 9) * N_TP + lax.shift_right_logical(column, 2)
    place = (column & (COLB - 1)) * ROWS + (row & (ROWS - 1))
    values = (
        lax.shift_right_logical(place, 7).astype(F32),
        (place & (LANES - 1)).astype(F32),
        ms_ref[...].astype(F32),
        vs_ref[...].astype(F32),
    )
    before = one_hot(iota((LANES, 2 * LANES), 0) < iota((LANES, 2 * LANES), 1))
    peer = iota((PEERS, LANES), 0)
    carry = jnp.zeros((PEERS, LANES), F32)
    side = jnp.zeros((PEERS, LANES), F32)
    slot_rows = []
    for k in range(CHUNKS):
        dest_row = dest[k : k + 1, :]
        hit = peer == dest_row
        counts = times(one_hot(hit), before)
        ahead = counts[:, :LANES] + carry
        carry = carry + counts[:, LANES:]
        rank = jnp.sum(jnp.where(hit, ahead, 0.0), axis=0, keepdims=True).astype(jnp.int32)
        slot_row = dest_row * PAIR + rank
        slot_rows.append(slot_row)
        slot_ref[k : k + 1, :] = slot_row
        ranked = iota((PAIR, LANES), 0) == rank
        table = jnp.concatenate(
            [jnp.where(ranked, v[k : k + 1, :], 0.0) for v in values]
            + [jnp.zeros((LANES - 4 * PAIR, LANES), F32)],
            axis=0,
        ).astype(BF16)
        side = side + lax.dot_general(
            one_hot(hit), table, (((1,), (1,)), ((), ())), preferred_element_type=F32
        )
    total = jnp.zeros((PAIR, grad_ref.shape[1]), F32)
    for k in range(ROWS // PAIR):
        g = grad_ref[k * PAIR : (k + 1) * PAIR, :].astype(F32)
        total = total + g * g
    total = jnp.sum(jnp.sum(total, axis=1, keepdims=True), axis=0, keepdims=True)
    high = total.astype(BF16).astype(F32)
    middle = (total - high).astype(BF16).astype(F32)
    low = total - high - middle
    lane = iota((PEERS, LANES), 1)
    side = jnp.where(lane == 64, high, side)
    side = jnp.where(lane == 65, middle, side)
    side = jnp.where(lane == 66, low, side).astype(BF16)
    spread = one_hot(
        lax.shift_right_logical(iota((PEERS * SIDE, PEERS), 0), 3) == iota((PEERS * SIDE, PEERS), 1)
    )
    msg_ref[:, pl.ds(MSG_ROWS, SIDE), :] = (
        times(spread, side).astype(BF16).reshape(PEERS, SIDE, LANES)
    )
    fill_message(msg_ref, slot_rows, codes_ref)


def prepare_v(slot_ref, codes_ref, msg_ref):
    slot = slot_ref[...]
    fill_message(msg_ref, [slot[k : k + 1, :] for k in range(CHUNKS)], codes_ref)


def received(msg_ref):
    return jnp.concatenate(
        [
            msg_ref[:, pl.ds(j * PAIR, PAIR), :].reshape(SAVED, LANES)
            for j in range(HALVES)
        ],
        axis=1,
    )


def decode_side(msg_ref):
    raw = msg_ref[:, pl.ds(MSG_ROWS, SIDE), :].reshape(PEERS * SIDE, LANES)
    gather = one_hot(iota((PEERS, PEERS * SIDE), 1) == iota((PEERS, PEERS * SIDE), 0) * SIDE)
    side = times(gather, raw)
    lane = iota((PEERS, LANES), 1)
    own = lax.shift_right_logical(lane, 4) == (iota((PEERS, LANES), 0) & 7)
    rows = []
    for q in range(4):
        widen = one_hot(
            iota((LANES, LANES), 0) == q * PAIR + (iota((LANES, LANES), 1) & (PAIR - 1))
        )
        wide = times(side.astype(BF16), widen)
        rows.append(jnp.sum(jnp.where(own, wide, 0.0).reshape(CHUNKS, 8, LANES), axis=1))
    sums = jnp.where((lane >= 64) & (lane < 67), side, 0.0)
    square_sum = jnp.sum(jnp.sum(sums, axis=1, keepdims=True), axis=0, keepdims=True)
    root_mean = jnp.sqrt(square_sum / (LAYERS * D * D) + guard)
    factor = jnp.minimum(1.0, clip_level / root_mean)
    place = (rows[0] * LANES + rows[1]).astype(jnp.int32)
    return place, rows[2], rows[3], factor


def as_row(column, count):
    rows = []
    diagonal = iota((LANES, LANES), 0) == iota((LANES, LANES), 1)
    for k in range(count // LANES):
        part = column[k * LANES : (k + 1) * LANES, :]
        rows.append(jnp.sum(jnp.where(diagonal, part, 0.0), axis=0, keepdims=True))
    return rows[0] if len(rows) == 1 else jnp.concatenate(rows, axis=1)


def scattered(place, scales, first, count, codes):
    place_rows = [place[k : k + 1, :] for k in range(CHUNKS)]
    scale_rows = [scales[k : k + 1, :] for k in range(CHUNKS)]
    matrix = jnp.concatenate(
        [picked_rows(place_rows, c * ROWS + first, count, scale_rows) for c in range(COLB)],
        axis=0,
    )
    return times(matrix, codes)


def update_m(msg_ref, grad_ref, m_ref, large_ref, step_ref, place_ref, vs_ref, factor_ref):
    count = grad_ref.shape[0]

    @pl.when(pl.program_id(0) == 0)
    def _():
        place, m_scales, v_scales, factor = decode_side(msg_ref)
        place_ref[...] = place
        vs_ref[0:CHUNKS, :] = v_scales
        vs_ref[CHUNKS:, :] = m_scales
        factor_ref[...] = jnp.broadcast_to(factor, factor_ref.shape)

    factor = factor_ref[0:1, 0:1]
    first = pl.program_id(0) * count
    previous = scattered(
        place_ref[...], vs_ref[CHUNKS:, :], first, count, received(msg_ref)
    )
    for c in range(COLB):
        columns = pl.ds(c * BLOCK, BLOCK)
        clipped = grad_ref[:, columns].astype(F32) * factor
        m_next = beta_one * previous[c * count : (c + 1) * count, :] + (1.0 - beta_one) * clipped
        largest = jnp.max(jnp.abs(m_next), axis=1, keepdims=True)
        m_ref[:, columns] = (m_next * (1.0 / (largest + guard))).astype(BF16)
        large_ref[c : c + 1, :] = as_row(largest, count)
        step_ref[:, columns] = m_next * (learn_rate / (1.0 - beta_one**step_count))


def update_v(
    msg_ref, grad_ref, param_ref, step_ref, place_ref, vs_ref, factor_ref, new_ref, v_ref, large_ref
):
    count = grad_ref.shape[0]
    factor = factor_ref[0:1, 0:1]
    first = pl.program_id(0) * count
    previous = scattered(
        place_ref[...], vs_ref[0:CHUNKS, :], first, count, received(msg_ref)
    )
    for c in range(COLB):
        columns = pl.ds(c * BLOCK, BLOCK)
        clipped = grad_ref[:, columns].astype(F32) * factor
        v_next = (
            beta_two * previous[c * count : (c + 1) * count, :]
            + (1.0 - beta_two) * clipped * clipped
        )
        largest = jnp.max(jnp.abs(v_next), axis=1, keepdims=True)
        v_ref[:, columns] = (v_next * (1.0 / (largest + guard))).astype(BF16)
        large_ref[c : c + 1, :] = as_row(largest, count)
        root = jnp.sqrt(v_next * (1.0 / (1.0 - beta_two**step_count)))
        new_ref[:, columns] = (
            param_ref[:, columns].astype(F32) - step_ref[:, columns] / (root + adam_eps)
        ).astype(BF16)


def shaped(shape, dtype):
    return jax.ShapeDtypeStruct(shape, dtype)


def whole(shape):
    return pl.BlockSpec(shape, lambda i: (0,) * len(shape))


TILE = 128


def body(param, grad, m_codes, v_codes, m_scales, v_scales, block_target):
    grad2 = grad.reshape(ROWS, COLB * BLOCK)
    param2 = param.reshape(ROWS, COLB * BLOCK)
    message_m, slot = pl.pallas_call(
        prepare_m,
        out_shape=(
            shaped((PEERS, MSG_ROWS + SIDE, LANES), BF16),
            shaped((CHUNKS, LANES), jnp.int32),
        ),
        name="prepare_m",
        interpret=INTERPRET,
    )(
        block_target.reshape(CHUNKS, LANES),
        m_scales.reshape(CHUNKS, LANES),
        v_scales.reshape(CHUNKS, LANES),
        grad2,
        m_codes,
    )
    got_m = lax.all_to_all(message_m, FSDP_TP, split_axis=0, concat_axis=0, tiled=True)
    message_v = pl.pallas_call(
        prepare_v,
        out_shape=shaped((PEERS, MSG_ROWS, LANES), BF16),
        name="prepare_v",
        interpret=INTERPRET,
    )(slot, v_codes)
    got_v = lax.all_to_all(message_v, FSDP_TP, split_axis=0, concat_axis=0, tiled=True)
    return finish(param2, grad2, got_m, got_v)


def finish(param2, grad2, got_m, got_v):
    wide = pl.BlockSpec((TILE, COLB * BLOCK), lambda i: (i, 0))
    scale_rows = pl.BlockSpec((COLB, TILE), lambda i: (0, i))
    m_quant, m_large, step, place, scales, factor = pl.pallas_call(
        update_m,
        grid=(ROWS // TILE,),
        in_specs=[whole(got_m.shape), wide],
        out_specs=[
            wide,
            scale_rows,
            wide,
            whole((CHUNKS, LANES)),
            whole((2 * CHUNKS, LANES)),
            whole((8, LANES)),
        ],
        out_shape=(
            shaped((ROWS, COLB * BLOCK), BF16),
            shaped((COLB, ROWS), F32),
            shaped((ROWS, COLB * BLOCK), F32),
            shaped((CHUNKS, LANES), jnp.int32),
            shaped((2 * CHUNKS, LANES), F32),
            shaped((8, LANES), F32),
        ),
        name="update_m",
        interpret=INTERPRET,
    )(got_m, grad2)
    new_param, v_quant, v_large = pl.pallas_call(
        update_v,
        grid=(ROWS // TILE,),
        in_specs=[
            whole(got_v.shape),
            wide,
            wide,
            wide,
            whole((CHUNKS, LANES)),
            whole((2 * CHUNKS, LANES)),
            whole((8, LANES)),
        ],
        out_specs=[wide, wide, scale_rows],
        out_shape=(
            shaped((ROWS, COLB * BLOCK), BF16),
            shaped((ROWS, COLB * BLOCK), BF16),
            shaped((COLB, ROWS), F32),
        ),
        name="update_v",
        interpret=INTERPRET,
    )(got_v, grad2, param2, step, place, scales, factor)
    return (
        new_param[None],
        m_quant[None],
        m_large.T[None],
        v_quant[None],
        v_large.T[None],
    )


def solution(mesh):
    torus = Mesh(
        mesh.devices.reshape(4, 2, 2, 4, 2), ("fsdp_0", "fsdp_1", "fsdp_2", "tp_0", "tp_1")
    )
    placed = (
        P(None, FSDP, TP),
        P(None, FSDP, TP),
        P(FSDP_TP, None),
        P(FSDP_TP, None),
        P(FSDP_TP),
        P(FSDP_TP),
        P(FSDP_TP),
    )
    return jax.shard_map(
        body,
        mesh=torus,
        in_specs=placed,
        out_specs=(
            P(None, FSDP, TP),
            P(None, FSDP, TP),
            P(None, FSDP, TP),
            P(None, FSDP, TP),
            P(None, FSDP, TP),
        ),
        check_vma=False,
    )
```

```python
import functools

import jax
import jax.numpy as jnp
from jax import lax
from jax.experimental import pallas as pl
from jax.experimental.pallas import tpu as pltpu
from jax.sharding import Mesh
from jax.sharding import PartitionSpec as P

D = 8192
LAYERS = 1
BLOCK = 256
FSDP = ("fsdp_0", "fsdp_1", "fsdp_2")
TP = ("tp_0", "tp_1")
FSDP_TP = ("fsdp_0", "fsdp_1", "fsdp_2", "tp_0", "tp_1")
SIZES = {"fsdp_0": 4, "fsdp_1": 2, "fsdp_2": 2, "tp_0": 4, "tp_1": 2}
EXCHANGE = ("fsdp_2", "fsdp_1", "tp_1", "tp_0", "fsdp_0")

PEERS = 128
PAIR = 16
SAVED = 2048
ROWS = 512
COLB = 4
LANES = 128
CHUNKS = SAVED // LANES
HALVES = BLOCK // LANES
MSG_ROWS = 2 * PAIR * HALVES
SIDE = 8
VMEM_LIMIT = 32 * 1024 * 1024

beta_one = 0.9
beta_two = 0.999
step_count = 1000.0
learn_rate = 0.002
clip_level = 0.5
guard = 1e-06
adam_eps = 1e-08

F32 = jnp.float32
BF16 = jnp.bfloat16


def iota(shape, dim):
    return lax.broadcasted_iota(jnp.int32, shape, dim)


def one_hot(condition):
    return jnp.where(condition, 1.0, 0.0).astype(BF16)


def times(a, b):
    return jnp.dot(a, b, preferred_element_type=F32)


def exchange_rank(fsdp, tp):
    place = {}
    for axes, index in ((FSDP, fsdp), (TP, tp)):
        for axis in reversed(axes):
            place[axis] = index & (SIZES[axis] - 1)
            index = lax.shift_right_logical(index, SIZES[axis].bit_length() - 1)
    rank = jnp.zeros_like(fsdp)
    for axis in EXCHANGE:
        rank = rank * SIZES[axis] + place[axis]
    return rank


def picked_rows(slot_rows, base, count, weights=None):
    wanted = iota((count, LANES), 0).astype(F32).astype(BF16)
    parts = []
    for k in range(CHUNKS):
        hit = wanted == (slot_rows[k] - base).astype(BF16)
        weight = jnp.ones((1, LANES), BF16) if weights is None else weights[k].astype(BF16)
        parts.append(jnp.where(hit, weight, jnp.zeros((1, LANES), BF16)))
    return jnp.concatenate(parts, axis=1)


def fill_message(msg_ref, slot_rows, m_codes, v_codes, tile=256):
    for t in range(SAVED // tile):
        matrix = picked_rows(slot_rows, float(t * tile), tile)
        first = t * tile // PAIR
        for part, codes in enumerate((m_codes, v_codes)):
            rows = times(matrix, codes).astype(BF16)
            for j in range(HALVES):
                msg_ref[
                    pl.ds(first, tile // PAIR), pl.ds((part * HALVES + j) * PAIR, PAIR), :
                ] = rows[:, j * LANES : (j + 1) * LANES].reshape(tile // PAIR, PAIR, LANES)


def prepare(target_hbm, ms_hbm, vs_hbm, grad_hbm, m_hbm, v_hbm, msg_ref, *scratch):
    refs, sem = scratch[:-1], scratch[-1]
    copies = [
        pltpu.make_async_copy(source, ref, sem.at[k])
        for k, (source, ref) in enumerate(
            zip((target_hbm, ms_hbm, vs_hbm, m_hbm, v_hbm, grad_hbm), refs)
        )
    ]
    for copy in copies:
        copy.start()
    target_ref, ms_ref, vs_ref, m_ref, v_ref, grad_ref = refs
    for copy in copies[:3]:
        copy.wait()
    target = target_ref[...]
    row = lax.shift_right_logical(target, 5)
    column = target & (D // BLOCK - 1)
    dest = exchange_rank(
        lax.shift_right_logical(row, 9), lax.shift_right_logical(column, 2)
    ).astype(F32)
    place = (column & (COLB - 1)) * ROWS + (row & (ROWS - 1))
    values = (
        lax.shift_right_logical(place, 7).astype(F32),
        (place & (LANES - 1)).astype(F32),
        ms_ref[...].astype(F32),
        vs_ref[...].astype(F32),
    )
    before = one_hot(iota((LANES, 2 * LANES), 0) < iota((LANES, 2 * LANES), 1))
    peer = iota((PEERS, LANES), 0).astype(F32)
    nth = iota((PAIR, LANES), 0).astype(F32)
    carry = jnp.zeros((PEERS, LANES), F32)
    side = jnp.zeros((PEERS, LANES), F32)
    slot_rows = []
    for k in range(CHUNKS):
        dest_row = dest[k : k + 1, :]
        hit = peer == dest_row
        hot = one_hot(hit)
        counts = times(hot, before)
        ahead = counts[:, :LANES] + carry
        carry = carry + counts[:, LANES:]
        rank = jnp.sum(jnp.where(hit, ahead, 0.0), axis=0, keepdims=True)
        slot_rows.append(dest_row * PAIR + rank)
        ranked = nth == rank
        table = jnp.concatenate(
            [jnp.where(ranked, v[k : k + 1, :], 0.0) for v in values]
            + [jnp.zeros((LANES - 4 * PAIR, LANES), F32)],
            axis=0,
        ).astype(BF16)
        side = side + lax.dot_general(
            hot, table, (((1,), (1,)), ((), ())), preferred_element_type=F32
        )
    for copy in copies[3:]:
        copy.wait()
    fill_message(msg_ref, slot_rows, m_ref[...], v_ref[...])
    total = jnp.zeros((PAIR, grad_ref.shape[1]), F32)
    for k in range(ROWS // PAIR):
        g = grad_ref[k * PAIR : (k + 1) * PAIR, :].astype(F32)
        total = total + g * g
    total = jnp.sum(jnp.sum(total, axis=1, keepdims=True), axis=0, keepdims=True)
    high = total.astype(BF16).astype(F32)
    middle = (total - high).astype(BF16).astype(F32)
    low = total - high - middle
    lane = iota((PEERS, LANES), 1)
    side = jnp.where(lane == 64, high, side)
    side = jnp.where(lane == 65, middle, side)
    side = jnp.where(lane == 66, low, side).astype(BF16)
    spread = one_hot(
        lax.shift_right_logical(iota((PEERS * SIDE, PEERS), 0), 3) == iota((PEERS * SIDE, PEERS), 1)
    )
    msg_ref[:, pl.ds(MSG_ROWS, SIDE), :] = (
        times(spread, side).astype(BF16).reshape(PEERS, SIDE, LANES)
    )


def received(msg_ref, part):
    return jnp.concatenate(
        [
            msg_ref[:, pl.ds((part * HALVES + j) * PAIR, PAIR), :].reshape(SAVED, LANES)
            for j in range(HALVES)
        ],
        axis=1,
    )


def decode_side(msg_ref):
    raw = msg_ref[:, pl.ds(MSG_ROWS, SIDE), :].reshape(PEERS * SIDE, LANES)
    gather = one_hot(iota((PEERS, PEERS * SIDE), 1) == iota((PEERS, PEERS * SIDE), 0) * SIDE)
    side = times(gather, raw)
    lane = iota((PEERS, LANES), 1)
    own = lax.shift_right_logical(lane, 4) == (iota((PEERS, LANES), 0) & 7)
    rows = []
    for q in range(4):
        widen = one_hot(
            iota((LANES, LANES), 0) == q * PAIR + (iota((LANES, LANES), 1) & (PAIR - 1))
        )
        wide = times(side.astype(BF16), widen)
        rows.append(jnp.sum(jnp.where(own, wide, 0.0).reshape(CHUNKS, 8, LANES), axis=1))
    sums = jnp.where((lane >= 64) & (lane < 67), side, 0.0)
    square_sum = jnp.sum(jnp.sum(sums, axis=1, keepdims=True), axis=0, keepdims=True)
    root_mean = jnp.sqrt(square_sum / (LAYERS * D * D) + guard)
    factor = jnp.minimum(1.0, clip_level / root_mean)
    place = rows[0] * LANES + rows[1]
    return place, rows[2], rows[3], factor


def as_row(column, count):
    rows = []
    diagonal = iota((LANES, LANES), 0) == iota((LANES, LANES), 1)
    for k in range(count // LANES):
        part = column[k * LANES : (k + 1) * LANES, :]
        rows.append(jnp.sum(jnp.where(diagonal, part, 0.0), axis=0, keepdims=True))
    return rows[0] if len(rows) == 1 else jnp.concatenate(rows, axis=1)


def scattered(place, scales, first, count, codes):
    place_rows = [place[k : k + 1, :] for k in range(CHUNKS)]
    scale_rows = [scales[k : k + 1, :] for k in range(CHUNKS)]
    matrix = jnp.concatenate(
        [
            picked_rows(place_rows, (c * ROWS + first).astype(F32), count, scale_rows)
            for c in range(COLB)
        ],
        axis=0,
    )
    return times(matrix, codes)


def update(
    msg_ref, grad_ref, param_ref, new_ref, m_ref, ml_ref, v_ref, vl_ref, place_ref, scale_ref, factor_ref
):
    count = new_ref.shape[0]

    @pl.when(pl.program_id(0) == 0)
    def _():
        place, m_scales, v_scales, factor = decode_side(msg_ref)
        place_ref[...] = place
        scale_ref[0, :, :] = m_scales
        scale_ref[1, :, :] = v_scales
        factor_ref[...] = jnp.broadcast_to(factor, factor_ref.shape)

    factor = factor_ref[0:1, 0:1]
    first = pl.program_id(0) * count
    place = place_ref[...]
    here = pl.ds(pl.multiple_of(first, count), count)
    m_prev = scattered(place, scale_ref[0, :, :], first, count, received(msg_ref, 0))
    v_prev = scattered(place, scale_ref[1, :, :], first, count, received(msg_ref, 1))
    for c in range(COLB):
        columns = pl.ds(c * BLOCK, BLOCK)
        part = slice(c * count, (c + 1) * count)
        clipped = grad_ref[here, columns].astype(F32) * factor
        m_next = beta_one * m_prev[part, :] + (1.0 - beta_one) * clipped
        largest = jnp.max(jnp.abs(m_next), axis=1, keepdims=True)
        m_ref[:, columns] = (m_next * (1.0 / (largest + guard))).astype(BF16)
        ml_ref[c : c + 1, :] = as_row(largest, count)
        v_next = beta_two * v_prev[part, :] + (1.0 - beta_two) * clipped * clipped
        largest = jnp.max(jnp.abs(v_next), axis=1, keepdims=True)
        v_ref[:, columns] = (v_next * (1.0 / (largest + guard))).astype(BF16)
        vl_ref[c : c + 1, :] = as_row(largest, count)
        root = jnp.sqrt(v_next * (1.0 / (1.0 - beta_two**step_count)))
        step = m_next * (learn_rate / (1.0 - beta_one**step_count)) / (root + adam_eps)
        new_ref[:, columns] = (param_ref[here, columns].astype(F32) - step).astype(BF16)


def shaped(shape, dtype):
    return jax.ShapeDtypeStruct(shape, dtype)


def whole(shape):
    return pl.BlockSpec(shape, lambda i: (0,) * len(shape))


TILE = 128


def make_message(grad2, m_codes, v_codes, m_scales, v_scales, block_target):
    arrays = (
        block_target.reshape(CHUNKS, LANES),
        m_scales.reshape(CHUNKS, LANES),
        v_scales.reshape(CHUNKS, LANES),
        grad2,
        m_codes,
        v_codes,
    )
    held = [arrays[k] for k in (0, 1, 2, 4, 5, 3)]
    return pl.pallas_call(
        prepare,
        in_specs=[pl.BlockSpec(memory_space=pltpu.HBM)] * len(arrays),
        out_shape=pltpu.VMEM((PEERS, MSG_ROWS + SIDE, LANES), BF16),
        scratch_shapes=[pltpu.VMEM(a.shape, a.dtype) for a in held]
        + [pltpu.SemaphoreType.DMA((len(held),))],
        name="prepare",
        compiler_params=pltpu.CompilerParams(vmem_limit_bytes=VMEM_LIMIT),
    )(*(pltpu.with_memory_space_constraint(a, pltpu.HBM) for a in arrays))


def finish(got, grad2, param2):
    wide = pl.BlockSpec((TILE, COLB * BLOCK), lambda i: (i, 0))
    scale_rows = pl.BlockSpec((COLB, TILE), lambda i: (0, i))
    matrix = shaped((ROWS, COLB * BLOCK), BF16)
    scales = shaped((COLB, ROWS), F32)
    return pl.pallas_call(
        update,
        grid=(ROWS // TILE,),
        in_specs=[pl.BlockSpec(memory_space=pltpu.VMEM)] * 3,
        out_specs=[wide, wide, scale_rows, wide, scale_rows],
        out_shape=(matrix, matrix, scales, matrix, scales),
        scratch_shapes=[
            pltpu.VMEM((CHUNKS, LANES), F32),
            pltpu.VMEM((2, CHUNKS, LANES), F32),
            pltpu.VMEM((8, LANES), F32),
        ],
        name="update",
        compiler_params=pltpu.CompilerParams(vmem_limit_bytes=VMEM_LIMIT),
    )(*(pltpu.with_memory_space_constraint(a, pltpu.VMEM) for a in (got, grad2, param2)))


def body(param, grad, m_codes, v_codes, m_scales, v_scales, block_target):
    grad2 = grad.reshape(ROWS, COLB * BLOCK)
    param2 = param.reshape(ROWS, COLB * BLOCK)
    message = make_message(grad2, m_codes, v_codes, m_scales, v_scales, block_target)
    got = lax.all_to_all(message, EXCHANGE, split_axis=0, concat_axis=0, tiled=True)
    new_param, m_quant, m_large, v_quant, v_large = finish(got, grad2, param2)
    return (
        new_param[None],
        m_quant[None],
        m_large.T[None],
        v_quant[None],
        v_large.T[None],
    )


def solution(mesh):
    torus = Mesh(
        mesh.devices.reshape(4, 2, 2, 4, 2), ("fsdp_0", "fsdp_1", "fsdp_2", "tp_0", "tp_1")
    )
    placed = (
        P(None, FSDP, TP),
        P(None, FSDP, TP),
        P(FSDP_TP, None),
        P(FSDP_TP, None),
        P(FSDP_TP),
        P(FSDP_TP),
        P(FSDP_TP),
    )
    return jax.shard_map(
        body,
        mesh=torus,
        in_specs=placed,
        out_specs=(
            P(None, FSDP, TP),
            P(None, FSDP, TP),
            P(None, FSDP, TP),
            P(None, FSDP, TP),
            P(None, FSDP, TP),
        ),
        check_vma=False,
    )
```

```python
import functools

import jax
import jax.numpy as jnp
from jax import lax
from jax.experimental import pallas as pl
from jax.experimental.pallas import tpu as pltpu
from jax.sharding import Mesh
from jax.sharding import PartitionSpec as P

D = 8192
LAYERS = 1
BLOCK = 256
FSDP = ("fsdp_0", "fsdp_1", "fsdp_2")
TP = ("tp_0", "tp_1")
FSDP_TP = ("fsdp_0", "fsdp_1", "fsdp_2", "tp_0", "tp_1")
SIZES = {"fsdp_0": 4, "fsdp_1": 2, "fsdp_2": 2, "tp_0": 4, "tp_1": 2}
EXCHANGE = ("fsdp_2", "fsdp_1", "tp_1", "tp_0", "fsdp_0")

PEERS = 128
PAIR = 16
SAVED = 2048
ROWS = 512
COLB = 4
LANES = 128
CHUNKS = SAVED // LANES
HALVES = BLOCK // LANES
MSG_ROWS = 2 * PAIR * HALVES
SIDE = 2
STRIDE = MSG_ROWS + SIDE
VMEM_LIMIT = 32 * 1024 * 1024

beta_one = 0.9
beta_two = 0.999
step_count = 1000.0
learn_rate = 0.002
clip_level = 0.5
guard = 1e-06
adam_eps = 1e-08

F32 = jnp.float32
BF16 = jnp.bfloat16


def iota(shape, dim):
    return lax.broadcasted_iota(jnp.int32, shape, dim)


def one_hot(condition):
    return jnp.where(condition, 1.0, 0.0).astype(BF16)


def times(a, b):
    return jnp.dot(a, b, preferred_element_type=F32)


def exchange_rank(fsdp, tp):
    place = {}
    for axes, index in ((FSDP, fsdp), (TP, tp)):
        for axis in reversed(axes):
            place[axis] = index & (SIZES[axis] - 1)
            index = lax.shift_right_logical(index, SIZES[axis].bit_length() - 1)
    rank = jnp.zeros_like(fsdp)
    for axis in EXCHANGE:
        rank = rank * SIZES[axis] + place[axis]
    return rank


def picked_rows(slot_rows, base, count, weights=None):
    wanted = iota((count, LANES), 0).astype(F32).astype(BF16)
    parts = []
    for k in range(CHUNKS):
        hit = wanted == (slot_rows[k] - base).astype(BF16)
        weight = jnp.ones((1, LANES), BF16) if weights is None else weights[k]
        parts.append(jnp.where(hit, weight, jnp.zeros((1, LANES), BF16)))
    return jnp.concatenate(parts, axis=1)


def fill_message(msg_ref, slot_rows, m_codes, v_codes, tile=512, step=256):
    for t in range(SAVED // tile):
        matrix = jnp.concatenate(
            [
                picked_rows(slot_rows, float(base), step)
                for base in range(t * tile, (t + 1) * tile, step)
            ],
            axis=0,
        )
        first = t * tile // PAIR
        for part, codes in enumerate((m_codes, v_codes)):
            rows = times(matrix, codes).astype(BF16)
            for j in range(HALVES):
                for p in range(tile // PAIR):
                    at = (first + p) * STRIDE + (part * HALVES + j) * PAIR
                    msg_ref[at : at + PAIR, :] = rows[
                        p * PAIR : (p + 1) * PAIR, j * LANES : (j + 1) * LANES
                    ]


def prepare(target_hbm, ms_hbm, vs_hbm, grad_hbm, m_hbm, v_hbm, msg_ref, *scratch):
    refs, sem = scratch[:-1], scratch[-1]
    copies = [
        pltpu.make_async_copy(source, ref, sem.at[k])
        for k, (source, ref) in enumerate(
            zip((target_hbm, ms_hbm, vs_hbm, grad_hbm, m_hbm, v_hbm), refs)
        )
    ]
    for copy in copies:
        copy.start()
    target_ref, ms_ref, vs_ref, grad_ref, m_ref, v_ref = refs
    for copy in copies[:3]:
        copy.wait()
    target = target_ref[...]
    row = lax.shift_right_logical(target, 5)
    column = target & (D // BLOCK - 1)
    dest = exchange_rank(
        lax.shift_right_logical(row, 9), lax.shift_right_logical(column, 2)
    ).astype(F32)
    place = (column & (COLB - 1)) * ROWS + (row & (ROWS - 1))
    values = (
        lax.shift_right_logical(place, 7).astype(F32),
        (place & (LANES - 1)).astype(F32),
        ms_ref[...].astype(F32),
        vs_ref[...].astype(F32),
    )
    before = one_hot(iota((LANES, 2 * LANES), 0) < iota((LANES, 2 * LANES), 1))
    peer = iota((PEERS, LANES), 0).astype(F32)
    nth = iota((PAIR, LANES), 0).astype(F32)
    carry = jnp.zeros((PEERS, LANES), F32)
    side = jnp.zeros((PEERS, LANES), F32)
    slot_rows = []
    total = jnp.zeros((8, grad_ref.shape[1]), F32)
    for k in range(CHUNKS):
        if k == CHUNKS // 2:
            copies[3].wait()
        if k >= CHUNKS // 2:
            share = 2 * ROWS // CHUNKS
            g = grad_ref[(k - CHUNKS // 2) * share : (k - CHUNKS // 2 + 1) * share, :].astype(F32)
            total = total + jnp.sum((g * g).reshape(-1, 8, g.shape[1]), axis=0)
        dest_row = dest[k : k + 1, :]
        hit = peer == dest_row
        hot = one_hot(hit)
        counts = times(hot, before)
        ahead = counts[:, :LANES] + carry
        carry = carry + counts[:, LANES:]
        rank = jnp.sum(jnp.where(hit, ahead, 0.0), axis=0, keepdims=True)
        slot_rows.append(dest_row * PAIR + rank)
        ranked = nth == rank
        table = jnp.concatenate(
            [jnp.where(ranked, v[k : k + 1, :], 0.0) for v in values]
            + [jnp.zeros((LANES - 4 * PAIR, LANES), F32)],
            axis=0,
        ).astype(BF16)
        side = side + lax.dot_general(
            hot, table, (((1,), (1,)), ((), ())), preferred_element_type=F32
        )
    total = jnp.sum(jnp.sum(total, axis=1, keepdims=True), axis=0, keepdims=True)
    high = total.astype(BF16).astype(F32)
    middle = (total - high).astype(BF16).astype(F32)
    low = total - high - middle
    lane = iota((PEERS, LANES), 1)
    side = jnp.where(lane == 64, high, side)
    side = jnp.where(lane == 65, middle, side)
    side = jnp.where(lane == 66, low, side).astype(BF16)
    spread = one_hot(
        lax.shift_right_logical(iota((PEERS * SIDE, PEERS), 0), 1) == iota((PEERS * SIDE, PEERS), 1)
    )
    side = times(spread, side).astype(BF16)
    for p in range(PEERS):
        at = p * STRIDE + MSG_ROWS
        msg_ref[at : at + SIDE, :] = side[p * SIDE : (p + 1) * SIDE, :]
    for copy in copies[4:]:
        copy.wait()
    fill_message(msg_ref, slot_rows, m_ref[...], v_ref[...])


def received(msg_ref, part):
    return jnp.concatenate(
        [
            jnp.concatenate(
                [
                    msg_ref[at : at + PAIR, :]
                    for at in range((part * HALVES + j) * PAIR, PEERS * STRIDE, STRIDE)
                ],
                axis=0,
            )
            for j in range(HALVES)
        ],
        axis=1,
    )


def decode_side(msg_ref):
    raw = jnp.concatenate(
        [
            msg_ref[at : at + PAIR, :]
            for at in range(STRIDE - PAIR, PEERS * STRIDE, STRIDE)
        ],
        axis=0,
    )
    gather = one_hot(
        iota((PEERS, PEERS * PAIR), 1) == iota((PEERS, PEERS * PAIR), 0) * PAIR + (PAIR - SIDE)
    )
    side = times(gather, raw)
    lane = iota((PEERS, LANES), 1)
    own = lax.shift_right_logical(lane, 4) == (iota((PEERS, LANES), 0) & 7)
    rows = []
    for q in range(4):
        widen = one_hot(
            iota((LANES, LANES), 0) == q * PAIR + (iota((LANES, LANES), 1) & (PAIR - 1))
        )
        wide = times(side.astype(BF16), widen)
        rows.append(jnp.sum(jnp.where(own, wide, 0.0).reshape(CHUNKS, 8, LANES), axis=1))
    sums = jnp.where((lane >= 64) & (lane < 67), side, 0.0)
    square_sum = jnp.sum(jnp.sum(sums, axis=1, keepdims=True), axis=0, keepdims=True)
    root_mean = jnp.sqrt(square_sum / (LAYERS * D * D) + guard)
    factor = jnp.minimum(1.0, clip_level / root_mean)
    place = rows[0] * LANES + rows[1]
    return place, rows[2], rows[3], factor


def as_row(column, count):
    rows = []
    diagonal = iota((LANES, LANES), 0) == iota((LANES, LANES), 1)
    for k in range(count // LANES):
        part = column[k * LANES : (k + 1) * LANES, :]
        rows.append(jnp.sum(jnp.where(diagonal, part, 0.0), axis=0, keepdims=True))
    return rows[0] if len(rows) == 1 else jnp.concatenate(rows, axis=1)


def scattered(place_rows, scale_rows, first, count, codes):
    matrix = jnp.concatenate(
        [
            picked_rows(place_rows, float(c * ROWS + first), count, scale_rows)
            for c in range(COLB)
        ],
        axis=0,
    )
    return times(matrix, codes)


def update(msg_ref, grad_ref, param_ref, *rest):
    outs, held, sem = rest[:5], rest[5:10], rest[10]
    new_ref, m_ref, ml_ref, v_ref, vl_ref = held
    place, m_scales, v_scales, factor = decode_side(msg_ref)
    place_rows = [place[k : k + 1, :] for k in range(CHUNKS)]
    m_rows = [m_scales[k : k + 1, :].astype(BF16) for k in range(CHUNKS)]
    v_rows = [v_scales[k : k + 1, :].astype(BF16) for k in range(CHUNKS)]
    m_codes, v_codes = received(msg_ref, 0), received(msg_ref, 1)
    gain = factor * (1.0 - beta_one)

    def previous(first):
        return (
            scattered(place_rows, m_rows, first, TILE, m_codes),
            scattered(place_rows, v_rows, first, TILE, v_codes),
        )

    def finish_tile(first, m_prev, v_prev):
        here = pl.ds(first, TILE)
        for c in range(COLB):
            columns = pl.ds(c * BLOCK, BLOCK)
            part = slice(c * TILE, (c + 1) * TILE)
            added = grad_ref[here, columns].astype(F32) * gain
            m_next = beta_one * m_prev[part, :] + added
            largest = jnp.max(jnp.abs(m_next), axis=1, keepdims=True)
            m_ref[here, columns] = (m_next * (1.0 / (largest + guard))).astype(BF16)
            ml_ref[c : c + 1, here] = as_row(largest, TILE)
            v_next = beta_two * v_prev[part, :] + added * added * (
                (1.0 - beta_two) / (1.0 - beta_one) ** 2
            )
            largest = jnp.max(v_next, axis=1, keepdims=True)
            v_ref[here, columns] = (v_next * (1.0 / (largest + guard))).astype(BF16)
            vl_ref[c : c + 1, here] = as_row(largest, TILE)
            square = v_next * (1.0 / (1.0 - beta_two**step_count))
            root = square * lax.rsqrt(square)
            step = m_next * (learn_rate / (1.0 - beta_one**step_count)) / (root + adam_eps)
            new_ref[here, columns] = (param_ref[here, columns].astype(F32) - step).astype(BF16)

    copies = []

    def send(k, here):
        copies.append(
            pltpu.make_async_copy(held[k].at[here], outs[k].at[here], sem.at[len(copies)])
        )
        copies[-1].start()

    ahead = previous(0)
    for first in range(0, ROWS, TILE):
        now = ahead
        if first + TILE < ROWS:
            ahead = previous(first + TILE)
        finish_tile(first, *now)
        for k in (0, 1, 3):
            send(k, pl.ds(first, TILE))
    for k in (2, 4):
        send(k, pl.ds(0, COLB))
    for copy in copies:
        copy.wait()


def shaped(shape, dtype):
    return jax.ShapeDtypeStruct(shape, dtype)


def whole(shape):
    return pl.BlockSpec(shape, lambda i: (0,) * len(shape))


TILE = 128


def make_message(grad2, m_codes, v_codes, m_scales, v_scales, block_target):
    arrays = (
        block_target.reshape(CHUNKS, LANES),
        m_scales.reshape(CHUNKS, LANES),
        v_scales.reshape(CHUNKS, LANES),
        grad2,
        m_codes,
        v_codes,
    )
    return pl.pallas_call(
        prepare,
        in_specs=[pl.BlockSpec(memory_space=pltpu.HBM)] * len(arrays),
        out_shape=pltpu.VMEM((PEERS * STRIDE, LANES), BF16),
        scratch_shapes=[pltpu.VMEM(a.shape, a.dtype) for a in arrays]
        + [pltpu.SemaphoreType.DMA((len(arrays),))],
        name="prepare",
        compiler_params=pltpu.CompilerParams(vmem_limit_bytes=VMEM_LIMIT),
    )(*(pltpu.with_memory_space_constraint(a, pltpu.HBM) for a in arrays))


def finish(got, grad2, param2):
    matrix = ((ROWS, COLB * BLOCK), BF16)
    scales = ((COLB, ROWS), F32)
    outs = (matrix, matrix, scales, matrix, scales)
    return pl.pallas_call(
        update,
        in_specs=[pl.BlockSpec(memory_space=pltpu.VMEM)] * 3,
        out_specs=[pl.BlockSpec(memory_space=pltpu.HBM)] * len(outs),
        out_shape=tuple(pltpu.HBM(*o) for o in outs),
        scratch_shapes=[pltpu.VMEM(*o) for o in outs]
        + [pltpu.SemaphoreType.DMA((3 * ROWS // TILE + 2,))],
        name="update",
        compiler_params=pltpu.CompilerParams(vmem_limit_bytes=VMEM_LIMIT),
    )(*(pltpu.with_memory_space_constraint(a, pltpu.VMEM) for a in (got, grad2, param2)))


def body(param, grad, m_codes, v_codes, m_scales, v_scales, block_target):
    grad2 = grad.reshape(ROWS, COLB * BLOCK)
    param2 = param.reshape(ROWS, COLB * BLOCK)
    message = make_message(grad2, m_codes, v_codes, m_scales, v_scales, block_target)
    pairs = message.reshape(PEERS, STRIDE // 2, 2, LANES)
    got = lax.all_to_all(pairs, EXCHANGE, split_axis=0, concat_axis=0, tiled=True)
    got = got.reshape(PEERS * STRIDE, LANES)
    new_param, m_quant, m_large, v_quant, v_large = finish(got, grad2, param2)
    return (
        new_param[None],
        m_quant[None],
        m_large.T[None],
        v_quant[None],
        v_large.T[None],
    )


def solution(mesh):
    torus = Mesh(
        mesh.devices.reshape(4, 2, 2, 4, 2), ("fsdp_0", "fsdp_1", "fsdp_2", "tp_0", "tp_1")
    )
    placed = (
        P(None, FSDP, TP),
        P(None, FSDP, TP),
        P(FSDP_TP, None),
        P(FSDP_TP, None),
        P(FSDP_TP),
        P(FSDP_TP),
        P(FSDP_TP),
    )
    return jax.shard_map(
        body,
        mesh=torus,
        in_specs=placed,
        out_specs=(
            P(None, FSDP, TP),
            P(None, FSDP, TP),
            P(None, FSDP, TP),
            P(None, FSDP, TP),
            P(None, FSDP, TP),
        ),
        check_vma=False,
    )
```

```python
import functools
import math

import jax
import jax.numpy as jnp
from jax import lax
from jax.experimental import pallas as pl
from jax.experimental.pallas import tpu as pltpu
from jax.sharding import Mesh
from jax.sharding import PartitionSpec as P

D = 8192
LAYERS = 1
BLOCK = 256
FSDP = ("fsdp_0", "fsdp_1", "fsdp_2")
TP = ("tp_0", "tp_1")
FSDP_TP = ("fsdp_0", "fsdp_1", "fsdp_2", "tp_0", "tp_1")
SIZES = {"fsdp_0": 4, "fsdp_1": 2, "fsdp_2": 2, "tp_0": 4, "tp_1": 2}
EXCHANGE = ("fsdp_2", "fsdp_1", "tp_1", "tp_0", "fsdp_0")

PEERS = 128
PAIR = 16
SAVED = 2048
ROWS = 512
COLB = 4
LANES = 128
CHUNKS = SAVED // LANES
HALVES = BLOCK // LANES
MSG_ROWS = 2 * PAIR * HALVES
SIDE = 2
STRIDE = MSG_ROWS + SIDE
VMEM_LIMIT = 32 * 1024 * 1024

beta_one = 0.9
beta_two = 0.999
step_count = 1000.0
learn_rate = 0.002
clip_level = 0.5
guard = 1e-06
adam_eps = 1e-08

M_UNIT = learn_rate * beta_one / (1.0 - beta_one**step_count)
V_UNIT = math.sqrt(beta_two / (1.0 - beta_two**step_count)) / M_UNIT

F32 = jnp.float32
BF16 = jnp.bfloat16


def iota(shape, dim):
    return lax.broadcasted_iota(jnp.int32, shape, dim)


def one_hot(condition):
    return jnp.where(condition, 1.0, 0.0).astype(BF16)


def times(a, b):
    return jnp.dot(a, b, preferred_element_type=F32)


def exchange_rank(fsdp, tp):
    place = {}
    for axes, index in ((FSDP, fsdp), (TP, tp)):
        for axis in reversed(axes):
            place[axis] = index & (SIZES[axis] - 1)
            index = lax.shift_right_logical(index, SIZES[axis].bit_length() - 1)
    rank = jnp.zeros_like(fsdp)
    for axis in EXCHANGE:
        rank = rank * SIZES[axis] + place[axis]
    return rank


def picked_rows(slot_rows, base, count, weights=None):
    wanted = iota((count, LANES), 0).astype(F32).astype(BF16)
    parts = []
    for k in range(CHUNKS):
        hit = wanted == (slot_rows[k] - base).astype(BF16)
        weight = jnp.ones((1, LANES), BF16) if weights is None else weights[k]
        parts.append(jnp.where(hit, weight, jnp.zeros((1, LANES), BF16)))
    return jnp.concatenate(parts, axis=1)


GROUP = 64
WIDE = 2 * LANES
TILES = SAVED // WIDE


def paired_rows(array):
    return paired([array[k : k + 1, :] for k in range(CHUNKS)])


def paired(rows):
    return jnp.concatenate(
        [jnp.concatenate(rows[k::2], axis=0) for k in range(2)], axis=1
    )


def grouped(target):
    tile = jnp.floor(target * (1.0 / WIDE))
    nth = iota((TILES, WIDE), 0).astype(F32)
    hit = jnp.concatenate([nth == tile[k : k + 1, :] for k in range(TILES)], axis=0)
    before = one_hot(iota((WIDE, WIDE), 0) < iota((WIDE, WIDE), 1))
    ahead = jnp.where(hit, times(one_hot(hit), before), 0.0)
    rank = jnp.sum(ahead.reshape(TILES, TILES, WIDE), axis=1)
    fits = jnp.max(rank) < GROUP - 0.5
    return target - tile * WIDE, tile * GROUP + rank, fits


def sort_chunks(row, labels, chunk_codes, held_ref):
    found = []
    for k in range(TILES):
        step = SAVED // TILES
        matrix = jnp.concatenate(
            [one_level(row[k : k + 1, :], float(base)) for base in (0, step)], axis=0
        )
        held_ref[:, k * GROUP : (k + 1) * GROUP, :] = (
            times(matrix, chunk_codes(k)).astype(BF16).reshape(TILES, GROUP, 2 * BLOCK)
        )
        table = jnp.concatenate(
            [v[k : k + 1, :] for v in labels] + [jnp.zeros((PAIR - len(labels), WIDE), F32)], axis=0
        ).astype(BF16)
        found.append(
            lax.dot_general(
                table, matrix, (((1,), (1,)), ((), ())), preferred_element_type=F32
            )
        )
    low = iota((TILES // 2, LANES), 1) < GROUP
    result = []
    for at in range(len(labels)):
        even = jnp.concatenate([f[at : at + 1, :] for f in found[0::2]], axis=0)
        odd = jnp.concatenate([f[at : at + 1, :] for f in found[1::2]], axis=0)
        rows = []
        for j in range(TILES // 2):
            lanes = slice(j * LANES, (j + 1) * LANES)
            rows.append(jnp.where(low, even[:, lanes], pltpu.roll(odd[:, lanes], GROUP, 1)))
            rows.append(jnp.where(low, pltpu.roll(even[:, lanes], GROUP, 1), odd[:, lanes]))
        result.append(rows)
    return result


def one_level(row, base, weight=None):
    wanted = iota((WIDE, row.shape[1]), 0).astype(F32).astype(BF16)
    hit = wanted == (row - base).astype(BF16)
    if weight is None:
        weight = jnp.ones((1, row.shape[1]), BF16)
    return jnp.where(hit, weight, jnp.zeros((1, row.shape[1]), BF16))


def second_level(places, weights=None):
    parts = []
    for q in range(TILES // 2):
        weight = None if weights is None else weights[q : q + 1, :].astype(BF16)
        parts.append(one_level(places[q : q + 1, :], 1.0, weight))
    return jnp.concatenate(parts, axis=1)


def fill_message_two(msg_ref, row, local, m_ref, v_ref, held_ref):
    def chunk_codes(k):
        here = pl.ds(k * WIDE, WIDE)
        return jnp.concatenate([m_ref[here, :], v_ref[here, :]], axis=1)

    (places,) = sort_chunks(row, (local + 1.0,), chunk_codes, held_ref)
    for t in range(TILES):
        rows = times(second_level(places[t]), held_ref[t]).astype(BF16)
        for p in range(WIDE // PAIR):
            for j in range(2 * HALVES):
                at = (t * WIDE // PAIR + p) * STRIDE + j * PAIR
                msg_ref[at : at + PAIR, :] = rows[
                    p * PAIR : (p + 1) * PAIR, j * LANES : (j + 1) * LANES
                ]


def fill_message(msg_ref, slot_rows, m_codes, v_codes, tile=512, step=256):
    for t in range(SAVED // tile):
        matrix = jnp.concatenate(
            [
                picked_rows(slot_rows, float(base), step)
                for base in range(t * tile, (t + 1) * tile, step)
            ],
            axis=0,
        )
        first = t * tile // PAIR
        for part, codes in enumerate((m_codes, v_codes)):
            rows = times(matrix, codes).astype(BF16)
            for j in range(HALVES):
                for p in range(tile // PAIR):
                    at = (first + p) * STRIDE + (part * HALVES + j) * PAIR
                    msg_ref[at : at + PAIR, :] = rows[
                        p * PAIR : (p + 1) * PAIR, j * LANES : (j + 1) * LANES
                    ]


def prepare(target_hbm, ms_hbm, vs_hbm, grad_hbm, m_hbm, v_hbm, msg_ref, *scratch):
    refs, held_ref, sem = scratch[:-2], scratch[-2], scratch[-1]
    copies = [
        pltpu.make_async_copy(source, ref, sem.at[k])
        for k, (source, ref) in enumerate(
            zip((target_hbm, ms_hbm, vs_hbm, grad_hbm, m_hbm, v_hbm), refs)
        )
    ]
    for copy in copies:
        copy.start()
    target_ref, ms_ref, vs_ref, grad_ref, m_ref, v_ref = refs
    for copy in copies[:3]:
        copy.wait()
    target = target_ref[...]
    row = lax.shift_right_logical(target, 5)
    column = target & (D // BLOCK - 1)
    dest = exchange_rank(
        lax.shift_right_logical(row, 9), lax.shift_right_logical(column, 2)
    ).astype(F32)
    place = (column & (COLB - 1)) * ROWS + (row & (ROWS - 1))
    values = (
        lax.shift_right_logical(place, 7).astype(F32),
        (place & (LANES - 1)).astype(F32),
        ms_ref[...].astype(F32),
        vs_ref[...].astype(F32),
    )
    lanes = (WIDE, WIDE + LANES)
    before = one_hot((iota(lanes, 0) < iota(lanes, 1)) | (iota(lanes, 1) >= WIDE))
    dest, values = paired_rows(dest), [paired_rows(v) for v in values]
    peer = iota((PEERS, WIDE), 0).astype(F32)
    nth = iota((PAIR, WIDE), 0).astype(F32)
    carry = jnp.zeros((PEERS, LANES), F32)
    side = jnp.zeros((PEERS, LANES), F32)
    slots = []
    total = jnp.zeros((8, grad_ref.shape[1]), F32)
    for k in range(TILES):
        if k == TILES // 2:
            copies[3].wait()
        if k >= TILES // 2:
            share = 2 * ROWS // TILES
            g = grad_ref[(k - TILES // 2) * share : (k - TILES // 2 + 1) * share, :].astype(F32)
            total = total + jnp.sum((g * g).reshape(-1, 8, g.shape[1]), axis=0)
        dest_row = dest[k : k + 1, :]
        hit = peer == dest_row
        hot = one_hot(hit)
        counts = times(hot, before)
        ahead = counts[:, :WIDE] + jnp.concatenate([carry, carry], axis=1)
        carry = carry + counts[:, WIDE:]
        rank = jnp.sum(jnp.where(hit, ahead, 0.0), axis=0, keepdims=True)
        slots.append(dest_row * PAIR + rank)
        ranked = nth == rank
        table = jnp.concatenate(
            [jnp.where(ranked, v[k : k + 1, :], 0.0) for v in values]
            + [jnp.zeros((LANES - 4 * PAIR, WIDE), F32)],
            axis=0,
        ).astype(BF16)
        side = side + lax.dot_general(
            hot, table, (((1,), (1,)), ((), ())), preferred_element_type=F32
        )
    total = jnp.sum(jnp.sum(total, axis=1, keepdims=True), axis=0, keepdims=True)
    high = total.astype(BF16).astype(F32)
    middle = (total - high).astype(BF16).astype(F32)
    low = total - high - middle
    lane = iota((PEERS, LANES), 1)
    side = jnp.where(lane == 64, high, side)
    side = jnp.where(lane == 65, middle, side)
    side = jnp.where(lane == 66, low, side).astype(BF16)
    spread = one_hot(
        lax.shift_right_logical(iota((PEERS * SIDE, PEERS), 0), 1) == iota((PEERS * SIDE, PEERS), 1)
    )
    side = times(spread, side).astype(BF16)
    for p in range(PEERS):
        at = p * STRIDE + MSG_ROWS
        msg_ref[at : at + SIDE, :] = side[p * SIDE : (p + 1) * SIDE, :]
    for copy in copies[4:]:
        copy.wait()
    local, row, fits = grouped(jnp.concatenate(slots, axis=0))

    @pl.when(fits)
    def _():
        fill_message_two(msg_ref, row, local, m_ref, v_ref, held_ref)

    @pl.when(jnp.logical_not(fits))
    def _():
        slot_rows = [
            slot[:, lanes] for slot in slots for lanes in (slice(0, LANES), slice(LANES, WIDE))
        ]
        fill_message(msg_ref, slot_rows, m_ref[...], v_ref[...])


def received(msg_ref, part):
    return jnp.concatenate(
        [
            jnp.concatenate(
                [
                    msg_ref[at : at + PAIR, :]
                    for at in range((part * HALVES + j) * PAIR, PEERS * STRIDE, STRIDE)
                ],
                axis=0,
            )
            for j in range(HALVES)
        ],
        axis=1,
    )


def decode_side(msg_ref):
    raw = jnp.concatenate(
        [
            msg_ref[at : at + PAIR, :]
            for at in range(STRIDE - PAIR, PEERS * STRIDE, STRIDE)
        ],
        axis=0,
    )
    gather = one_hot(
        iota((PEERS, PEERS * PAIR), 1) == iota((PEERS, PEERS * PAIR), 0) * PAIR + (PAIR - SIDE)
    )
    side = times(gather, raw)
    lane = iota((PEERS, LANES), 1)
    own = lax.shift_right_logical(lane, 4) == (iota((PEERS, LANES), 0) & 7)
    rows = []
    for q in range(4):
        widen = one_hot(
            iota((LANES, LANES), 0) == q * PAIR + (iota((LANES, LANES), 1) & (PAIR - 1))
        )
        wide = times(side.astype(BF16), widen)
        rows.append(jnp.sum(jnp.where(own, wide, 0.0).reshape(CHUNKS, 8, LANES), axis=1))
    sums = jnp.where((lane >= 64) & (lane < 67), side, 0.0)
    square_sum = jnp.sum(jnp.sum(sums, axis=1, keepdims=True), axis=0, keepdims=True)
    root_mean = jnp.sqrt(square_sum / (LAYERS * D * D) + guard)
    factor = jnp.minimum(1.0, clip_level / root_mean)
    place = rows[0] * LANES + rows[1]
    return place, rows[2], rows[3], factor


def as_row(column, count):
    rows = []
    diagonal = iota((LANES, LANES), 0) == iota((LANES, LANES), 1)
    for k in range(count // LANES):
        part = column[k * LANES : (k + 1) * LANES, :]
        rows.append(jnp.sum(jnp.where(diagonal, part, 0.0), axis=0, keepdims=True))
    return rows[0] if len(rows) == 1 else jnp.concatenate(rows, axis=1)


def received_chunk(msg_ref, k):
    first = k * (WIDE // PAIR) * STRIDE
    return jnp.concatenate(
        [
            jnp.concatenate(
                [
                    msg_ref[at : at + PAIR, :]
                    for at in range(
                        first + j * PAIR, first + j * PAIR + (WIDE // PAIR) * STRIDE, STRIDE
                    )
                ],
                axis=0,
            )
            for j in range(2 * HALVES)
        ],
        axis=1,
    )


def update(msg_ref, grad_ref, param_ref, *rest):
    outs, held, held_ref, sem = rest[:5], rest[5:10], rest[10], rest[11]
    new_ref, m_ref, ml_ref, v_ref, vl_ref = held
    place, m_scales, v_scales, factor = decode_side(msg_ref)
    place_rows = [place[k : k + 1, :] for k in range(CHUNKS)]
    m_rows = [m_scales[k : k + 1, :] for k in range(CHUNKS)]
    v_rows = [v_scales[k : k + 1, :] for k in range(CHUNKS)]
    m_gain = factor * ((1.0 - beta_one) / beta_one)
    v_gain = factor * math.sqrt((1.0 - beta_two) / beta_two)
    local, row, fits = grouped(paired(place_rows))

    def finish_tile(t, m_prev, v_prev):
        here = pl.ds((t % HALF) * WIDE, WIDE)
        c = t // HALF
        columns = pl.ds(c * BLOCK, BLOCK)
        g = grad_ref[here, columns].astype(F32)
        m_part = m_prev + g * m_gain
        largest = jnp.max(jnp.abs(m_part), axis=1, keepdims=True)
        m_ref[here, columns] = (m_part * (1.0 / (largest + guard / beta_one))).astype(BF16)
        ml_ref[c : c + 1, here] = as_row(largest, WIDE) * beta_one
        v_root = g * v_gain
        v_part = v_prev + v_root * v_root
        largest = jnp.max(v_part, axis=1, keepdims=True)
        v_ref[here, columns] = (v_part * (1.0 / (largest + guard / beta_two))).astype(BF16)
        vl_ref[c : c + 1, here] = as_row(largest, WIDE) * beta_two
        root = v_part * lax.rsqrt(v_part) * V_UNIT + adam_eps / M_UNIT
        new_ref[here, columns] = (param_ref[here, columns].astype(F32) - m_part / root).astype(BF16)

    def run(previous):
        copies = []

        def send(k, here):
            copies.append(
                pltpu.make_async_copy(held[k].at[here], outs[k].at[here], sem.at[len(copies)])
            )
            copies[-1].start()

        order = [c * HALF + h for h in range(HALF) for c in range(COLB)]
        ahead = previous(order[0])
        for at, t in enumerate(order):
            now = ahead
            if at + 1 < len(order):
                ahead = previous(order[at + 1])
            finish_tile(t, *now)
            for k in (0, 1, 3):
                send(k, (pl.ds((t % HALF) * WIDE, WIDE), pl.ds(t // HALF * BLOCK, BLOCK)))
        for k in (2, 4):
            send(k, pl.ds(0, COLB))
        for copy in copies:
            copy.wait()

    @pl.when(fits)
    def _():
        labels = (local + 1.0, paired(m_rows), paired(v_rows))
        places, m_weights, v_weights = sort_chunks(
            row, labels, functools.partial(received_chunk, msg_ref), held_ref
        )

        def previous(t):
            return (
                times(second_level(places[t], m_weights[t]), held_ref[t, :, :BLOCK]),
                times(second_level(places[t], v_weights[t]), held_ref[t, :, BLOCK:]),
            )

        run(previous)

    @pl.when(jnp.logical_not(fits))
    def _():
        def previous(t):
            return tuple(
                times(
                    picked_rows(
                        place_rows, float(t * WIDE), WIDE, [w.astype(BF16) for w in weights]
                    ),
                    received(msg_ref, part),
                )
                for part, weights in enumerate((m_rows, v_rows))
            )

        run(previous)


def shaped(shape, dtype):
    return jax.ShapeDtypeStruct(shape, dtype)


def whole(shape):
    return pl.BlockSpec(shape, lambda i: (0,) * len(shape))


HALF = ROWS // WIDE


def make_message(grad2, m_codes, v_codes, m_scales, v_scales, block_target):
    arrays = (
        block_target.reshape(CHUNKS, LANES),
        m_scales.reshape(CHUNKS, LANES),
        v_scales.reshape(CHUNKS, LANES),
        grad2,
        m_codes,
        v_codes,
    )
    return pl.pallas_call(
        prepare,
        in_specs=[pl.BlockSpec(memory_space=pltpu.HBM)] * len(arrays),
        out_shape=pltpu.VMEM((PEERS * STRIDE, LANES), BF16),
        scratch_shapes=[pltpu.VMEM(a.shape, a.dtype) for a in arrays]
        + [pltpu.VMEM((TILES, TILES * GROUP, 2 * BLOCK), BF16)]
        + [pltpu.SemaphoreType.DMA((len(arrays),))],
        name="prepare",
        compiler_params=pltpu.CompilerParams(vmem_limit_bytes=VMEM_LIMIT),
    )(*(pltpu.with_memory_space_constraint(a, pltpu.HBM) for a in arrays))


def finish(got, grad2, param2):
    matrix = ((ROWS, COLB * BLOCK), BF16)
    scales = ((COLB, ROWS), F32)
    outs = (matrix, matrix, scales, matrix, scales)
    return pl.pallas_call(
        update,
        in_specs=[pl.BlockSpec(memory_space=pltpu.VMEM)] * 3,
        out_specs=[pl.BlockSpec(memory_space=pltpu.HBM)] * len(outs),
        out_shape=tuple(pltpu.HBM(*o) for o in outs),
        scratch_shapes=[pltpu.VMEM(*o) for o in outs]
        + [
            pltpu.VMEM((TILES, TILES * GROUP, 2 * BLOCK), BF16),
            pltpu.SemaphoreType.DMA((3 * TILES + 2,)),
        ],
        name="update",
        compiler_params=pltpu.CompilerParams(vmem_limit_bytes=VMEM_LIMIT),
    )(*(pltpu.with_memory_space_constraint(a, pltpu.VMEM) for a in (got, grad2, param2)))


def body(param, grad, m_codes, v_codes, m_scales, v_scales, block_target):
    grad2 = grad.reshape(ROWS, COLB * BLOCK)
    param2 = param.reshape(ROWS, COLB * BLOCK)
    message = make_message(grad2, m_codes, v_codes, m_scales, v_scales, block_target)
    pairs = message.reshape(PEERS, STRIDE // 2, 2, LANES)
    got = lax.all_to_all(pairs, EXCHANGE, split_axis=0, concat_axis=0, tiled=True)
    got = got.reshape(PEERS * STRIDE, LANES)
    new_param, m_quant, m_large, v_quant, v_large = finish(got, grad2, param2)
    return (
        new_param[None],
        m_quant[None],
        m_large.T[None],
        v_quant[None],
        v_large.T[None],
    )


def solution(mesh):
    torus = Mesh(
        mesh.devices.reshape(4, 2, 2, 4, 2), ("fsdp_0", "fsdp_1", "fsdp_2", "tp_0", "tp_1")
    )
    placed = (
        P(None, FSDP, TP),
        P(None, FSDP, TP),
        P(FSDP_TP, None),
        P(FSDP_TP, None),
        P(FSDP_TP),
        P(FSDP_TP),
        P(FSDP_TP),
    )
    return jax.shard_map(
        body,
        mesh=torus,
        in_specs=placed,
        out_specs=(
            P(None, FSDP, TP),
            P(None, FSDP, TP),
            P(None, FSDP, TP),
            P(None, FSDP, TP),
            P(None, FSDP, TP),
        ),
        check_vma=False,
    )
```

```python
import functools
import math

import jax
import jax.numpy as jnp
from jax import lax
from jax.experimental import pallas as pl
from jax.experimental.pallas import tpu as pltpu
from jax.sharding import Mesh
from jax.sharding import PartitionSpec as P

D = 8192
LAYERS = 1
BLOCK = 256
FSDP = ("fsdp_0", "fsdp_1", "fsdp_2")
TP = ("tp_0", "tp_1")
FSDP_TP = ("fsdp_0", "fsdp_1", "fsdp_2", "tp_0", "tp_1")
SIZES = {"fsdp_0": 4, "fsdp_1": 2, "fsdp_2": 2, "tp_0": 4, "tp_1": 2}
EXCHANGE = ("fsdp_2", "fsdp_1", "tp_1", "tp_0", "fsdp_0")

PEERS = 128
PAIR = 16
SAVED = 2048
ROWS = 512
COLB = 4
LANES = 128
CHUNKS = SAVED // LANES
HALVES = BLOCK // LANES
MSG_ROWS = 2 * PAIR * HALVES
SIDE = 2
STRIDE = MSG_ROWS + SIDE
VMEM_LIMIT = 32 * 1024 * 1024

beta_one = 0.9
beta_two = 0.999
step_count = 1000.0
learn_rate = 0.002
clip_level = 0.5
guard = 1e-06
adam_eps = 1e-08

M_UNIT = learn_rate * beta_one / (1.0 - beta_one**step_count)
V_UNIT = math.sqrt(beta_two / (1.0 - beta_two**step_count)) / M_UNIT

F32 = jnp.float32
BF16 = jnp.bfloat16


def iota(shape, dim):
    return lax.broadcasted_iota(jnp.int32, shape, dim)


def one_hot(condition):
    return jnp.where(condition, 1.0, 0.0).astype(BF16)


def times(a, b):
    return jnp.dot(a, b, preferred_element_type=F32)


def exchange_rank(fsdp, tp):
    place = {}
    for axes, index in ((FSDP, fsdp), (TP, tp)):
        for axis in reversed(axes):
            place[axis] = index & (SIZES[axis] - 1)
            index = lax.shift_right_logical(index, SIZES[axis].bit_length() - 1)
    rank = jnp.zeros_like(fsdp)
    for axis in EXCHANGE:
        rank = rank * SIZES[axis] + place[axis]
    return rank


def picked_rows(slot_rows, base, count, weights=None):
    wanted = iota((count, LANES), 0).astype(F32).astype(BF16)
    parts = []
    for k in range(CHUNKS):
        hit = wanted == (slot_rows[k] - base).astype(BF16)
        weight = jnp.ones((1, LANES), BF16) if weights is None else weights[k]
        parts.append(jnp.where(hit, weight, jnp.zeros((1, LANES), BF16)))
    return jnp.concatenate(parts, axis=1)


GROUP = 64
WIDE = 2 * LANES
TILES = SAVED // WIDE


def paired_rows(array):
    return paired([array[k : k + 1, :] for k in range(CHUNKS)])


def paired(rows):
    return jnp.concatenate(
        [jnp.concatenate(rows[k::2], axis=0) for k in range(2)], axis=1
    )


def grouped(target):
    tile = jnp.floor(target * (1.0 / WIDE))
    nth = iota((TILES, WIDE), 0).astype(F32)
    hit = jnp.concatenate([nth == tile[k : k + 1, :] for k in range(TILES)], axis=0)
    before = one_hot(iota((WIDE, WIDE), 0) < iota((WIDE, WIDE), 1))
    ahead = jnp.where(hit, times(one_hot(hit), before), 0.0)
    rank = jnp.sum(ahead.reshape(TILES, TILES, WIDE), axis=1)
    fits = jnp.max(rank) < GROUP - 0.5
    return target - tile * WIDE, tile * GROUP + rank, fits


def sort_chunks(row, labels, chunk_codes, held_ref, label_ref):
    found = []
    for k in range(TILES):
        step = SAVED // TILES
        matrix = jnp.concatenate(
            [one_level(row[k : k + 1, :], float(base)) for base in (0, step)], axis=0
        )
        held_ref[:, k * GROUP : (k + 1) * GROUP, :] = (
            times(matrix, chunk_codes(k)).astype(BF16).reshape(TILES, GROUP, 2 * BLOCK)
        )
        table = jnp.concatenate(
            [v[k : k + 1, :] for v in labels] + [jnp.zeros((PAIR - len(labels), WIDE), F32)], axis=0
        ).astype(BF16)
        found.append(
            lax.dot_general(
                table, matrix, (((1,), (1,)), ((), ())), preferred_element_type=F32
            )
        )
    low = iota((TILES // 2, LANES), 1) < GROUP
    for at in range(len(labels)):
        even = jnp.concatenate([f[at : at + 1, :] for f in found[0::2]], axis=0)
        odd = jnp.concatenate([f[at : at + 1, :] for f in found[1::2]], axis=0)
        for j in range(TILES // 2):
            lanes = slice(j * LANES, (j + 1) * LANES)
            label_ref[at, 2 * j] = jnp.where(
                low, even[:, lanes], pltpu.roll(odd[:, lanes], GROUP, 1)
            )
            label_ref[at, 2 * j + 1] = jnp.where(
                low, pltpu.roll(even[:, lanes], GROUP, 1), odd[:, lanes]
            )


def one_level(row, base, weight=None):
    wanted = iota((WIDE, row.shape[1]), 0).astype(F32).astype(BF16)
    hit = wanted == (row - base).astype(BF16)
    if weight is None:
        weight = jnp.ones((1, row.shape[1]), BF16)
    return jnp.where(hit, weight, jnp.zeros((1, row.shape[1]), BF16))


def second_level(places, weights=None):
    parts = []
    for q in range(TILES // 2):
        weight = None if weights is None else weights[q : q + 1, :].astype(BF16)
        parts.append(one_level(places[q : q + 1, :], 1.0, weight))
    return jnp.concatenate(parts, axis=1)


def fill_message_two(msg_ref, held_ref, label_ref):
    for t in range(TILES):
        rows = times(second_level(label_ref[0, t]), held_ref[t]).astype(BF16)
        for p in range(WIDE // PAIR):
            for j in range(2 * HALVES):
                at = (t * WIDE // PAIR + p) * STRIDE + j * PAIR
                msg_ref[at : at + PAIR, :] = rows[
                    p * PAIR : (p + 1) * PAIR, j * LANES : (j + 1) * LANES
                ]


def fill_message(msg_ref, slot_rows, m_codes, v_codes, tile=512, step=256):
    for t in range(SAVED // tile):
        matrix = jnp.concatenate(
            [
                picked_rows(slot_rows, float(base), step)
                for base in range(t * tile, (t + 1) * tile, step)
            ],
            axis=0,
        )
        first = t * tile // PAIR
        for part, codes in enumerate((m_codes, v_codes)):
            rows = times(matrix, codes).astype(BF16)
            for j in range(HALVES):
                for p in range(tile // PAIR):
                    at = (first + p) * STRIDE + (part * HALVES + j) * PAIR
                    msg_ref[at : at + PAIR, :] = rows[
                        p * PAIR : (p + 1) * PAIR, j * LANES : (j + 1) * LANES
                    ]


def prepare(target_hbm, ms_hbm, vs_hbm, grad_hbm, m_hbm, v_hbm, msg_ref, *scratch):
    refs, (held_ref, label_ref, sem) = scratch[:-3], scratch[-3:]
    copies = [
        pltpu.make_async_copy(source, ref, sem.at[k])
        for k, (source, ref) in enumerate(
            zip((target_hbm, ms_hbm, vs_hbm, grad_hbm, m_hbm, v_hbm), refs)
        )
    ]
    for copy in copies:
        copy.start()
    target_ref, ms_ref, vs_ref, grad_ref, m_ref, v_ref = refs
    lanes = (WIDE, WIDE + LANES)
    before = one_hot((iota(lanes, 0) < iota(lanes, 1)) | (iota(lanes, 1) >= WIDE))
    for copy in copies[:3]:
        copy.wait()
    target = target_ref[...]
    row = lax.shift_right_logical(target, 5)
    column = target & (D // BLOCK - 1)
    dest = exchange_rank(
        lax.shift_right_logical(row, 9), lax.shift_right_logical(column, 2)
    ).astype(F32)
    place = (column & (COLB - 1)) * ROWS + (row & (ROWS - 1))
    values = (
        lax.shift_right_logical(place, 7).astype(F32),
        (place & (LANES - 1)).astype(F32),
        ms_ref[...].astype(F32),
        vs_ref[...].astype(F32),
    )
    dest, values = paired_rows(dest), [paired_rows(v) for v in values]
    peer = iota((PEERS, WIDE), 0).astype(F32)
    nth = iota((PAIR, WIDE), 0).astype(F32)
    carry = jnp.zeros((PEERS, LANES), F32)
    side = jnp.zeros((PEERS, LANES), F32)
    slots = []
    for k in range(TILES):
        dest_row = dest[k : k + 1, :]
        hit = peer == dest_row
        hot = one_hot(hit)
        counts = times(hot, before)
        ahead = counts[:, :WIDE] + jnp.concatenate([carry, carry], axis=1)
        carry = carry + counts[:, WIDE:]
        rank = jnp.sum(jnp.where(hit, ahead, 0.0), axis=0, keepdims=True)
        slots.append(dest_row * PAIR + rank)
        ranked = nth == rank
        table = jnp.concatenate(
            [jnp.where(ranked, v[k : k + 1, :], 0.0) for v in values]
            + [jnp.zeros((LANES - 4 * PAIR, WIDE), F32)],
            axis=0,
        ).astype(BF16)
        side = side + lax.dot_general(
            hot, table, (((1,), (1,)), ((), ())), preferred_element_type=F32
        )
    local, row, fits = grouped(jnp.concatenate(slots, axis=0))
    for copy in copies[3:]:
        copy.wait()

    def squares(k):
        share = ROWS // TILES
        g = grad_ref[k * share : (k + 1) * share, :].astype(F32)
        return jnp.sum((g * g).reshape(-1, 8, g.shape[1]), axis=0)

    def fill_side(total):
        total = jnp.sum(jnp.sum(total, axis=1, keepdims=True), axis=0, keepdims=True)
        high = total.astype(BF16).astype(F32)
        middle = (total - high).astype(BF16).astype(F32)
        low = total - high - middle
        lane = iota((PEERS, LANES), 1)
        whole_side = jnp.where(lane == 64, high, side)
        whole_side = jnp.where(lane == 65, middle, whole_side)
        whole_side = jnp.where(lane == 66, low, whole_side).astype(BF16)
        spread = one_hot(
            lax.shift_right_logical(iota((PEERS * SIDE, PEERS), 0), 1)
            == iota((PEERS * SIDE, PEERS), 1)
        )
        doubled = times(spread, whole_side).astype(BF16)
        for p in range(PEERS):
            at = p * STRIDE + MSG_ROWS
            msg_ref[at : at + SIDE, :] = doubled[p * SIDE : (p + 1) * SIDE, :]

    @pl.when(fits)
    def _():
        sums = []

        def chunk_codes(k):
            sums.append(squares(k))
            here = pl.ds(k * WIDE, WIDE)
            return jnp.concatenate([m_ref[here, :], v_ref[here, :]], axis=1)

        sort_chunks(row, (local + 1.0,), chunk_codes, held_ref, label_ref)
        fill_side(sum(sums[1:], sums[0]))

    @pl.when(fits)
    def _():
        fill_message_two(msg_ref, held_ref, label_ref)

    @pl.when(jnp.logical_not(fits))
    def _():
        sums = [squares(k) for k in range(TILES)]
        fill_side(sum(sums[1:], sums[0]))
        slot_rows = [
            slot[:, lanes] for slot in slots for lanes in (slice(0, LANES), slice(LANES, WIDE))
        ]
        fill_message(msg_ref, slot_rows, m_ref[...], v_ref[...])


def received(msg_ref, part):
    return jnp.concatenate(
        [
            jnp.concatenate(
                [
                    msg_ref[at : at + PAIR, :]
                    for at in range((part * HALVES + j) * PAIR, PEERS * STRIDE, STRIDE)
                ],
                axis=0,
            )
            for j in range(HALVES)
        ],
        axis=1,
    )


def decode_side(msg_ref):
    raw = jnp.concatenate(
        [msg_ref[at : at + SIDE, :] for at in range(MSG_ROWS, PEERS * STRIDE, STRIDE)], axis=0
    )
    gather = one_hot(iota((PEERS, PEERS * SIDE), 1) == iota((PEERS, PEERS * SIDE), 0) * SIDE)
    side = times(gather, raw)
    lane = iota((PEERS, LANES), 1)
    own = lax.shift_right_logical(lane, 4) == (iota((PEERS, LANES), 0) & 7)
    field = (LANES, 4 * LANES)
    widen = one_hot(
        iota(field, 0)
        == lax.shift_right_logical(iota(field, 1), 7) * PAIR + (iota(field, 1) & (PAIR - 1))
    )
    wide = times(side.astype(BF16), widen)
    rows = [
        jnp.sum(
            jnp.where(own, wide[:, q * LANES : (q + 1) * LANES], 0.0).reshape(CHUNKS, 8, LANES),
            axis=1,
        )
        for q in range(4)
    ]
    sums = jnp.where((lane >= 64) & (lane < 67), side, 0.0)
    square_sum = jnp.sum(jnp.sum(sums, axis=1, keepdims=True), axis=0, keepdims=True)
    root_mean = jnp.sqrt(square_sum / (LAYERS * D * D) + guard)
    factor = jnp.minimum(1.0, clip_level / root_mean)
    place = rows[0] * LANES + rows[1]
    return place, rows[2], rows[3], factor


def as_row(column, count):
    rows = []
    diagonal = iota((LANES, LANES), 0) == iota((LANES, LANES), 1)
    for k in range(count // LANES):
        part = column[k * LANES : (k + 1) * LANES, :]
        rows.append(jnp.sum(jnp.where(diagonal, part, 0.0), axis=0, keepdims=True))
    return rows[0] if len(rows) == 1 else jnp.concatenate(rows, axis=1)


def received_chunk(msg_ref, k):
    first = k * (WIDE // PAIR) * STRIDE
    return jnp.concatenate(
        [
            jnp.concatenate(
                [
                    msg_ref[at : at + PAIR, :]
                    for at in range(
                        first + j * PAIR, first + j * PAIR + (WIDE // PAIR) * STRIDE, STRIDE
                    )
                ],
                axis=0,
            )
            for j in range(2 * HALVES)
        ],
        axis=1,
    )


def update(msg_ref, grad_ref, param_ref, *rest):
    outs, held, held_ref, label_ref, gm_ref, gv_ref, sem = rest[:5], rest[5:10], *rest[10:]
    new_ref, m_ref, ml_ref, v_ref, vl_ref = held
    place, m_scales, v_scales, factor = decode_side(msg_ref)
    place_rows = [place[k : k + 1, :] for k in range(CHUNKS)]
    m_rows = [m_scales[k : k + 1, :] for k in range(CHUNKS)]
    v_rows = [v_scales[k : k + 1, :] for k in range(CHUNKS)]
    m_gain = factor * ((1.0 - beta_one) / beta_one)
    v_gain = factor * math.sqrt((1.0 - beta_two) / beta_two)
    local, row, fits = grouped(paired(place_rows))

    def gradient_terms(k):
        here = pl.ds(k * (ROWS // TILES), ROWS // TILES)
        g = grad_ref[here, :].astype(F32)
        v_root = g * v_gain
        gm_ref[here, :] = g * m_gain
        gv_ref[here, :] = v_root * v_root

    def finish_tile(t, m_prev, v_prev):
        here = pl.ds((t % HALF) * WIDE, WIDE)
        c = t // HALF
        columns = pl.ds(c * BLOCK, BLOCK)
        m_part = m_prev + gm_ref[here, columns]
        largest = jnp.max(jnp.abs(m_part), axis=1, keepdims=True)
        m_ref[here, columns] = (m_part * (1.0 / (largest + guard / beta_one))).astype(BF16)
        ml_ref[c : c + 1, here] = as_row(largest, WIDE) * beta_one
        v_part = v_prev + gv_ref[here, columns]
        largest = jnp.max(v_part, axis=1, keepdims=True)
        v_ref[here, columns] = (v_part * (1.0 / (largest + guard / beta_two))).astype(BF16)
        vl_ref[c : c + 1, here] = as_row(largest, WIDE) * beta_two
        root = v_part * lax.rsqrt(v_part) * V_UNIT + adam_eps / M_UNIT
        new_ref[here, columns] = (param_ref[here, columns].astype(F32) - m_part / root).astype(BF16)

    def run(previous):
        copies = []

        def send(k, here):
            copies.append(
                pltpu.make_async_copy(held[k].at[here], outs[k].at[here], sem.at[len(copies)])
            )
            copies[-1].start()

        order = [c * HALF + h for h in range(HALF) for c in range(COLB)]
        ahead = previous(order[0])
        for at, t in enumerate(order):
            now = ahead
            if at + 1 < len(order):
                ahead = previous(order[at + 1])
            finish_tile(t, *now)
            for k in (0, 1, 3):
                send(k, (pl.ds((t % HALF) * WIDE, WIDE), pl.ds(t // HALF * BLOCK, BLOCK)))
        for k in (2, 4):
            send(k, pl.ds(0, COLB))
        for copy in copies:
            copy.wait()

    @pl.when(fits)
    def _():
        labels = (local + 1.0, paired(m_rows), paired(v_rows))

        def chunk_codes(k):
            gradient_terms(k)
            return received_chunk(msg_ref, k)

        sort_chunks(row, labels, chunk_codes, held_ref, label_ref)

    @pl.when(fits)
    def _():
        def previous(t):
            places = label_ref[0, t]
            return (
                times(second_level(places, label_ref[1, t]), held_ref[t, :, :BLOCK]),
                times(second_level(places, label_ref[2, t]), held_ref[t, :, BLOCK:]),
            )

        run(previous)

    @pl.when(jnp.logical_not(fits))
    def _():
        for k in range(TILES):
            gradient_terms(k)

        def previous(t):
            return tuple(
                times(
                    picked_rows(
                        place_rows, float(t * WIDE), WIDE, [w.astype(BF16) for w in weights]
                    ),
                    received(msg_ref, part),
                )
                for part, weights in enumerate((m_rows, v_rows))
            )

        run(previous)


def shaped(shape, dtype):
    return jax.ShapeDtypeStruct(shape, dtype)


def whole(shape):
    return pl.BlockSpec(shape, lambda i: (0,) * len(shape))


HALF = ROWS // WIDE


def make_message(grad2, m_codes, v_codes, m_scales, v_scales, block_target):
    arrays = (
        block_target.reshape(CHUNKS, LANES),
        m_scales.reshape(CHUNKS, LANES),
        v_scales.reshape(CHUNKS, LANES),
        grad2,
        m_codes,
        v_codes,
    )
    return pl.pallas_call(
        prepare,
        in_specs=[pl.BlockSpec(memory_space=pltpu.HBM)] * len(arrays),
        out_shape=pltpu.VMEM((PEERS * STRIDE, LANES), BF16),
        scratch_shapes=[pltpu.VMEM(a.shape, a.dtype) for a in arrays]
        + [pltpu.VMEM((TILES, TILES * GROUP, 2 * BLOCK), BF16)]
        + [pltpu.VMEM((1, TILES, TILES // 2, LANES), F32)]
        + [pltpu.SemaphoreType.DMA((len(arrays),))],
        name="prepare",
        compiler_params=pltpu.CompilerParams(vmem_limit_bytes=VMEM_LIMIT),
    )(*(pltpu.with_memory_space_constraint(a, pltpu.HBM) for a in arrays))


def finish(got, grad2, param2):
    matrix = ((ROWS, COLB * BLOCK), BF16)
    scales = ((COLB, ROWS), F32)
    outs = (matrix, matrix, scales, matrix, scales)
    return pl.pallas_call(
        update,
        in_specs=[pl.BlockSpec(memory_space=pltpu.VMEM)] * 3,
        out_specs=[pl.BlockSpec(memory_space=pltpu.HBM)] * len(outs),
        out_shape=tuple(pltpu.HBM(*o) for o in outs),
        scratch_shapes=[pltpu.VMEM(*o) for o in outs]
        + [
            pltpu.VMEM((TILES, TILES * GROUP, 2 * BLOCK), BF16),
            pltpu.VMEM((3, TILES, TILES // 2, LANES), F32),
            pltpu.VMEM((ROWS, COLB * BLOCK), F32),
            pltpu.VMEM((ROWS, COLB * BLOCK), F32),
            pltpu.SemaphoreType.DMA((3 * TILES + 2,)),
        ],
        name="update",
        compiler_params=pltpu.CompilerParams(vmem_limit_bytes=VMEM_LIMIT),
    )(*(pltpu.with_memory_space_constraint(a, pltpu.VMEM) for a in (got, grad2, param2)))


def body(param, grad, m_codes, v_codes, m_scales, v_scales, block_target):
    grad2 = grad.reshape(ROWS, COLB * BLOCK)
    param2 = param.reshape(ROWS, COLB * BLOCK)
    message = make_message(grad2, m_codes, v_codes, m_scales, v_scales, block_target)
    pairs = message.reshape(PEERS, STRIDE // 2, 2, LANES)
    got = lax.all_to_all(pairs, EXCHANGE, split_axis=0, concat_axis=0, tiled=True)
    got = got.reshape(PEERS * STRIDE, LANES)
    new_param, m_quant, m_large, v_quant, v_large = finish(got, grad2, param2)
    return (
        new_param[None],
        m_quant[None],
        m_large.T[None],
        v_quant[None],
        v_large.T[None],
    )


def solution(mesh):
    torus = Mesh(
        mesh.devices.reshape(4, 2, 2, 4, 2), ("fsdp_0", "fsdp_1", "fsdp_2", "tp_0", "tp_1")
    )
    placed = (
        P(None, FSDP, TP),
        P(None, FSDP, TP),
        P(FSDP_TP, None),
        P(FSDP_TP, None),
        P(FSDP_TP),
        P(FSDP_TP),
        P(FSDP_TP),
    )
    return jax.shard_map(
        body,
        mesh=torus,
        in_specs=placed,
        out_specs=(
            P(None, FSDP, TP),
            P(None, FSDP, TP),
            P(None, FSDP, TP),
            P(None, FSDP, TP),
            P(None, FSDP, TP),
        ),
        check_vma=False,
    )
```
